8 devices in a mesh: dp: 1 (over z), ep: 8 (over x, y, core).
Axes of the slice: x: 2, y: 2, z: 1, core: 2. Of those that a mesh axis runs over, the one named last changes fastest.
Arguments:
- x: bfloat16 [1, 8, 256, 7168], P('dp', 'ep')
- expert: int32 [1, 8, 256, 8], P('dp', 'ep')
- slot: int32 [1, 8, 256, 8], P('dp', 'ep')
- gate: float32 [1, 8, 256, 8], P('dp', 'ep')
- w_gate: bfloat16 [24, 7168, 2048], P('ep')
- w_up: bfloat16 [24, 7168, 2048], P('ep')
- w_down: bfloat16 [24, 2048, 7168], P('ep')
- s_gate: bfloat16 [7168, 2048], replicated
- s_up: bfloat16 [7168, 2048], replicated
- s_down: bfloat16 [2048, 7168], replicated
Outputs:
- y: bfloat16 [1, 8, 256, 7168], P('dp', 'ep')
All inputs are finite; a program needn't handle non-finite values.
Results may differ from the reference program's by a relative error of at most 0.009.
Values are sent between devices in bfloat16 or wider.
A program may use at most 2 GiB of HBM per device.

```python
import jax
import jax.numpy as jnp

MEMBERS = 8
TOKENS = 256
D = 7168
FF = 2048
TOP = 8
EXPERTS = 24
SHARED_FF = 2048
SLOTS = 5 * TOKENS * TOP // (4 * EXPERTS)


def setup_inputs(seed: int = 0, part: int = 0) -> dict:
    own, k1, k2, k3, k4, k5, k6 = jax.random.split(jax.random.key(seed), 7)
    kx, ke, kl, kg = jax.random.split(jax.random.fold_in(own, part), 4)
    devices = (1, MEMBERS)
    place = jax.random.permutation(kl, jnp.arange(EXPERTS, dtype=jnp.uint32))
    slow = ((EXPERTS + (9 * place) % EXPERTS) << ((9 * place) // EXPERTS)) // EXPERTS
    wait = (jax.random.bits(ke, (*devices, TOKENS, EXPERTS), jnp.uint32) >> 10) * slow
    expert = jnp.argsort(wait, axis=-1)[..., :TOP].astype(jnp.int32)
    chosen = jax.nn.one_hot(expert, EXPERTS, dtype=jnp.int32)
    in_line = jnp.cumsum(chosen.reshape(*devices, TOKENS * TOP, EXPERTS), axis=2) - 1
    slot = jnp.sum(in_line.reshape(chosen.shape) * chosen, axis=-1)

    def one(key, rows, columns):
        return (jax.random.normal(key, (rows, columns), jnp.float32) * rows**-0.5).astype(jnp.bfloat16)

    def weights(key, rows, columns):
        return jax.lax.map(lambda k: one(k, rows, columns), jax.random.split(key, EXPERTS))

    return {
        "x": jax.random.normal(kx, (*devices, TOKENS, D), jnp.float32).astype(jnp.bfloat16),
        "expert": expert,
        "slot": slot,
        "gate": jax.nn.softmax(jax.random.normal(kg, expert.shape, jnp.float32)),
        "w_gate": weights(k1, D, FF),
        "w_up": weights(k2, D, FF),
        "w_down": weights(k3, FF, D),
        "s_gate": one(k4, D, SHARED_FF),
        "s_up": one(k5, D, SHARED_FF),
        "s_down": one(k6, SHARED_FF, D),
    }


def einsum(form, a, b):
    return jnp.einsum(form, a.astype(jnp.float32), b.astype(jnp.float32))


def for_all(x, s_gate, s_up, s_down):
    h = jax.nn.silu(einsum("...d,df->...f", x, s_gate)) * einsum("...d,df->...f", x, s_up)
    return einsum("...f,fd->...d", h.astype(jnp.bfloat16), s_down)


def reference(x, expert, slot, gate, w_gate, w_up, w_down, s_gate, s_up, s_down):
    to_expert = jax.nn.one_hot(expert, EXPERTS, dtype=jnp.bfloat16)
    to_slot = jax.nn.one_hot(slot, SLOTS, dtype=jnp.bfloat16)
    weighted = to_expert * gate[..., None].astype(jnp.bfloat16)
    dispatch = einsum("abtke,abtkc->abtec", to_expert, to_slot).astype(jnp.bfloat16)
    combine = einsum("abtke,abtkc->abtec", weighted, to_slot).astype(jnp.bfloat16)
    z = einsum("abtec,abtd->aebcd", dispatch, x).astype(jnp.bfloat16)
    h = jax.nn.silu(einsum("aebcd,edf->aebcf", z, w_gate))
    h = (h * einsum("aebcd,edf->aebcf", z, w_up)).astype(jnp.bfloat16)
    out = einsum("aebcf,efd->aebcd", h, w_down).astype(jnp.bfloat16)
    y = einsum("abtec,aebcd->abtd", combine, out)
    return (y + for_all(x, s_gate, s_up, s_down)).astype(jnp.bfloat16)
```

```python
import jax
import jax.numpy as jnp
from jax import lax
from jax.sharding import PartitionSpec as P

F32, BF16 = jnp.float32, jnp.bfloat16
CHUNKS = 4


def dot(a, b):
    return lax.dot_general(a, b, (((a.ndim - 1,), (b.ndim - 2,)), ((), ())), preferred_element_type=F32)


def bdot(a, b):
    return lax.dot_general(a, b, (((2,), (1,)), ((0,), (0,))), preferred_element_type=F32)


def solution(mesh):
    n = mesh.shape["ep"]

    def to(bit, v):
        return lax.ppermute(v, "ep", [(i, i ^ bit) for i in range(n)])

    def local(x, expert, slot, gate, w_gate, w_up, w_down, s_gate, s_up, s_down):
        me = lax.axis_index("ep")
        x, expert, slot, gate = x[0, 0], expert[0, 0], slot[0, 0], gate[0, 0]
        tokens, top = expert.shape
        depth = x.shape[1]
        own = w_gate.shape[0]
        slots = 5 * tokens * top // (4 * own * n)
        half = tokens // 2

        xs = {0: x, 1: to(1, x), 2: to(2, x), 4: to(4, x)}
        xs[3], xs[5] = to(1, xs[2]), to(1, xs[4])
        xs[6] = jnp.concatenate([to(2, xs[4][:half]), to(4, xs[2][half:])], axis=0)
        xs[7] = to(1, xs[6])

        place = jnp.where(slot < slots, expert * slots + slot, -1)
        place = lax.all_gather(place, "ep")
        weight = lax.all_gather(gate, "ep").astype(BF16)
        seats = me * own * slots + jnp.arange(own * slots)

        def maps(bits):
            p = lax.dynamic_index_in_dim(place, me ^ bits, 0, keepdims=False)
            g = lax.dynamic_index_in_dim(weight, me ^ bits, 0, keepdims=False)
            hit = p[:, :, None] == seats
            return (
                jnp.any(hit, axis=1).astype(BF16).T,
                jnp.sum(jnp.where(hit, g[:, :, None].astype(F32), 0.0), axis=1).astype(BF16),
            )

        sel = {b: maps(b) for b in range(n)}

        def up(group):
            z = [dot(sel[b][0], xs[b]).astype(BF16).reshape(own, slots, depth) for b in group]
            z = jnp.concatenate(z, axis=1)
            return (jax.nn.silu(bdot(z, w_gate)) * bdot(z, w_up)).astype(BF16)

        hs = (jax.nn.silu(dot(x, s_gate)) * dot(x, s_up)).astype(BF16)
        shared = dot(hs, s_down)
        groups = ((0, 1), (2, 3, 4, 5), (6, 7))
        h = jnp.concatenate([up(g) for g in groups], axis=1)
        order = [b for g in groups for b in g]

        ys = []
        width = depth // CHUNKS
        for c in range(CHUNKS):
            cols = slice(c * width, (c + 1) * width)
            out = bdot(h, w_down[:, :, cols]).astype(BF16).reshape(own, n, slots, width)

            def term(b):
                return dot(sel[b][1], out[:, order.index(b)].reshape(own * slots, width))

            pair = to(1, jnp.stack([term(b ^ 1).astype(BF16) for b in (6, 4, 2, 0)]))
            pair = dict(zip((6, 4, 2, 0), pair.astype(F32)))
            far = (term(6) + pair[6]).astype(BF16)
            via_x, via_y = to(4, far[:half]).astype(F32), to(2, far[half:]).astype(F32)
            none = jnp.zeros_like(via_x)
            from_y = to(2, (term(2) + pair[2] + jnp.concatenate([via_x, none])).astype(BF16))
            from_x = to(4, (term(4) + pair[4] + jnp.concatenate([none, via_y])).astype(BF16))
            y = term(0) + pair[0] + from_x.astype(F32) + from_y.astype(F32) + shared[:, cols]
            ys.append(y.astype(BF16))
        return jnp.concatenate(ys, axis=1)[None, None]

    tok, exp, rep = P("dp", "ep"), P("ep"), P()
    return jax.shard_map(
        local,
        mesh=mesh,
        in_specs=(tok, tok, tok, tok, exp, exp, exp, rep, rep, rep),
        out_specs=tok,
        check_vma=False,
    )
```

```python
import functools

import jax
import jax.numpy as jnp
from jax import lax
from jax.experimental import pallas as pl
from jax.experimental.pallas import tpu as pltpu
from jax.sharding import PartitionSpec as P

F32, BF16 = jnp.float32, jnp.bfloat16
VMEM_LIMIT = 62 * 2**20
WIN = 112
TILE = 512


def dot(a, b):
    return lax.dot_general(a, b, (((a.ndim - 1,), (b.ndim - 2,)), ((), ())), preferred_element_type=F32)


def remote(src, dst, left, here, device):
    return pltpu.make_async_remote_copy(
        src_ref=src,
        dst_ref=dst,
        send_sem=left,
        recv_sem=here,
        device_id={"ep": device},
        device_id_type=pl.DeviceIdType.MESH,
    )


def others():
    me = lax.axis_index("ep")
    return me + 1 - 2 * (me % 2), me + 2 - 4 * ((me // 2) % 2), me + 4 - 8 * ((me // 4) % 2)


def meet(barrier, devices):
    for device in devices:
        pl.semaphore_signal(barrier, inc=1, device_id={"ep": device}, device_id_type=pl.DeviceIdType.MESH)
    pl.semaphore_wait(barrier, len(devices))


def dispatch(pos_ref, i, x_ref, z_ref, at):
    pos = pos_ref[pl.ds(i, 1), :]
    hot = (lax.broadcasted_iota(jnp.int32, (WIN, pos.shape[1]), 0) == pos).astype(F32).astype(BF16)
    for k in range(0, z_ref.shape[1], 512):
        z_ref[at : at + WIN, k : k + 512] = dot(hot, x_ref[:, k : k + 512]).astype(BF16)


def gather_kernel(own, n, plan, pos_ref, x_ref, sg_ref, su_ref, wg_ref, wu_ref, *refs):
    hs_ref, h_ref, g_ref, u_ref, far_ref, xp_ref, xr_ref, zp_ref, zr_ref, ga_ref, ua_ref = refs[:11]
    pair_left, pair_here, left, here = refs[11:]
    shared, pairs, rest, per = plan
    i = pl.program_id(0)
    depth = wg_ref.shape[1]
    half = x_ref.shape[0] // 2
    partner, beside_y, beside_x = others()
    barrier = pltpu.get_barrier_semaphore()

    def block(c, q):
        return xr_ref.at[q] if c == 0 else far_ref.at[q]

    def copy(c, k):
        if k < 2:
            src, dst, device = x_ref.at[:, pl.ds(c * depth, depth)], block(c, 2 * k), (beside_y, beside_x)[k]
        elif k == 2:
            src, dst, device = block(c, 2).at[pl.ds(0, half)], block(c, 4).at[pl.ds(0, half)], beside_y
        elif k == 3:
            src, dst, device = block(c, 0).at[pl.ds(half, half)], block(c, 4).at[pl.ds(half, half)], beside_x
        else:
            src, dst, device = block(c, 2 * k - 8), block(c, 2 * k - 7), partner
        return remote(src, dst, left.at[c, k], here.at[c, k], device)

    pair = remote(x_ref, xp_ref, pair_left.at[0], pair_here.at[0], partner)

    @pl.when(i == 0)
    def _():
        meet(barrier, (partner, beside_y, beside_x))
        copy(0, 0).start()
        copy(0, 1).start()
        pair.start()

    def forward(c):
        copy(c, 0).wait_recv()
        copy(c, 1).wait_recv()
        for k in (2, 3, 4, 5):
            copy(c, k).start()

    def onward(c):
        copy(c, 2).wait_recv()
        copy(c, 3).wait_recv()
        copy(c, 6).start()

    def arrived(c):
        for k in (4, 5, 6):
            copy(c, k).wait_recv()

    @pl.when(i == shared + 10)
    def _():
        forward(0)
        copy(1, 0).start()
        copy(1, 1).start()

    @pl.when(i == shared + 20)
    def _():
        onward(0)

    @pl.when(i == shared + pairs + 5)
    def _():
        forward(1)

    @pl.when(i == shared + pairs + 9)
    def _():
        onward(1)

    def two_halves(k, z_ref, ws, rows, cols, store):
        for part in range(2):

            @pl.when(k == part)
            def _():
                z = z_ref[:rows, part * depth : (part + 1) * depth]
                g, u = dot(z, ws[0]), dot(z, ws[1])
                if part == 0:
                    ga_ref[:rows, :cols] = g
                    ua_ref[:rows, :cols] = u
                else:
                    g, u = g + ga_ref[:rows, :cols], u + ua_ref[:rows, :cols]
                    store((jax.nn.silu(g) * u).astype(BF16))

    @pl.when(i < shared)
    def _():
        def store(v):
            hs_ref[...] = v

        two_halves(i % 2, x_ref, (sg_ref[...], su_ref[...]), x_ref.shape[0], sg_ref.shape[1], store)

    @pl.when((i >= shared) & (i < shared + pairs))
    def _():
        p = i - shared

        @pl.when(p == 0)
        def _():
            pair.wait_recv()

        @pl.when(p % (2 * per) == 0)
        def _():
            e = p // (2 * per)
            dispatch(pos_ref, e, x_ref, zp_ref, 0)
            dispatch(pos_ref, own + e, xp_ref, zp_ref, WIN)

        def store(v):
            h_ref[0] = v

        two_halves(p % 2, zp_ref, (wg_ref[0], wu_ref[0]), 2 * WIN, wg_ref.shape[2], store)

    @pl.when(i >= shared + pairs)
    def _():
        r = i - shared - pairs

        @pl.when(r == 0)
        def _():
            arrived(0)

        @pl.when(r % per == 0)
        def _():
            for q in range(n - 2):
                dispatch(pos_ref, (q + 2) * own + r // per, xr_ref.at[q], zr_ref, q * WIN)

        rows = zr_ref.shape[0] // 2
        for m in (0, rows):
            z = zr_ref[m : m + rows, :]
            g_ref[0, m : m + rows, :] = dot(z, wg_ref[0])
            u_ref[0, m : m + rows, :] = dot(z, wu_ref[0])

    @pl.when(i == shared + pairs + rest - 1)
    def _():
        arrived(1)
        pair.wait_send()
        for c in range(2):
            for k in range(7):
                copy(c, k).wait_send()


def gather(x, pos, s_gate, s_up, w_gate, w_up):
    tokens, depth = x.shape
    own, _, ff = w_gate.shape
    n = pos.shape[0] // own
    half = depth // 2
    per = ff // TILE
    narrow = TILE // 2
    shared, pairs, rest = 2 * s_gate.shape[1] // narrow, 2 * own * per, own * per
    rows = (n - 2) * WIN
    one = pl.Buffered(1)

    def whole(v):
        return pl.BlockSpec(v.shape, lambda i: (0,) * v.ndim, pipeline_mode=one)

    def s_at(i):
        i = jnp.minimum(i, shared - 1)
        return i % 2, i // 2

    def w_at(i):
        p = jnp.clip(i - shared, 0, pairs - 1)
        r = jnp.maximum(i - shared - pairs, 0)
        late = i >= shared + pairs
        return (
            jnp.where(late, r // per, p // (2 * per)),
            jnp.where(late, 0, p % 2),
            jnp.where(late, r % per, p // 2 % per),
        )

    def h_at(i):
        p = jnp.clip(i - shared, 0, pairs - 1)
        return p // (2 * per), 0, p // 2 % per

    def a_at(i):
        r = jnp.maximum(i - shared - pairs, 0)
        return r // per, 0, r % per

    s_spec = pl.BlockSpec((half, narrow), s_at)
    w_spec = pl.BlockSpec((1, half, TILE), w_at)
    a_spec = pl.BlockSpec((1, rows, TILE), a_at)
    wide = jax.ShapeDtypeStruct((own, rows, ff), F32)
    dma = pltpu.SemaphoreType.DMA
    flops = 4 * (tokens * s_gate.shape[1] + own * (2 * WIN + rows // 2) * ff) * depth
    return pl.pallas_call(
        functools.partial(gather_kernel, own, n, (shared, pairs, rest, per)),
        out_shape=(
            jax.ShapeDtypeStruct((tokens, s_gate.shape[1]), BF16),
            jax.ShapeDtypeStruct((own, 2 * WIN, ff), BF16),
            wide,
            wide,
            jax.ShapeDtypeStruct((n - 2, tokens, half), BF16),
        ),
        grid=(shared + pairs + rest,),
        in_specs=[whole(pos), whole(x), s_spec, s_spec, w_spec, w_spec],
        out_specs=(
            pl.BlockSpec((tokens, narrow), lambda i: (0, jnp.minimum(i, shared - 1) // 2)),
            pl.BlockSpec((1, 2 * WIN, TILE), h_at),
            a_spec,
            a_spec,
            pl.BlockSpec(memory_space=pl.ANY),
        ),
        scratch_shapes=[
            pltpu.VMEM((tokens, depth), BF16),
            pltpu.VMEM((n - 2, tokens, half), BF16),
            pltpu.VMEM((2 * WIN, depth), BF16),
            pltpu.VMEM((rows, half), BF16),
            pltpu.VMEM((tokens, TILE), F32),
            pltpu.VMEM((tokens, TILE), F32),
            dma((1,)),
            dma((1,)),
            dma((2, 7)),
            dma((2, 7)),
        ],
        compiler_params=pltpu.CompilerParams(
            vmem_limit_bytes=VMEM_LIMIT, collective_id=1, has_side_effects=True
        ),
        cost_estimate=pl.CostEstimate(flops=flops, bytes_accessed=own * 2 * depth * ff * 2, transcendentals=0),
        name="gather",
    )(pos, x, s_gate, s_up, w_gate, w_up)


def rest_kernel(own, pos_ref, x_ref, wg_ref, wu_ref, g_ref, u_ref, h_ref, z_ref):
    e = pl.program_id(0)

    @pl.when(pl.program_id(1) == 0)
    def _():
        for q in range(x_ref.shape[0]):
            dispatch(pos_ref, (q + 2) * own + e, x_ref.at[q], z_ref, q * WIN)

    rows = z_ref.shape[0] // 2
    for m in (0, rows):
        z = z_ref[m : m + rows, :]
        g = dot(z, wg_ref[0]) + g_ref[0, m : m + rows, :]
        u = dot(z, wu_ref[0]) + u_ref[0, m : m + rows, :]
        h_ref[0, m : m + rows, :] = (jax.nn.silu(g) * u).astype(BF16)


def finish(pos, x, w_gate, w_up, g, u):
    own, rows, ff = g.shape
    half = x.shape[2]
    one = pl.Buffered(1)

    def whole(v):
        return pl.BlockSpec(v.shape, lambda e, j: (0,) * v.ndim, pipeline_mode=one)

    w_spec = pl.BlockSpec((1, half, TILE), lambda e, j: (e, 1, j))
    a_spec = pl.BlockSpec((1, rows, TILE), lambda e, j: (e, 0, j))
    return pl.pallas_call(
        functools.partial(rest_kernel, own),
        out_shape=jax.ShapeDtypeStruct((own, rows, ff), BF16),
        grid=(own, ff // TILE),
        in_specs=[whole(pos), whole(x), w_spec, w_spec, a_spec, a_spec],
        out_specs=a_spec,
        scratch_shapes=[pltpu.VMEM((rows, half), BF16)],
        compiler_params=pltpu.CompilerParams(vmem_limit_bytes=VMEM_LIMIT),
        cost_estimate=pl.CostEstimate(
            flops=4 * own * rows * half * ff, bytes_accessed=4 * own * half * ff, transcendentals=0
        ),
        name="finish",
    )(pos, x, w_gate, w_up, g, u)


def down_kernel(n, own, tiles, pos_ref, gate_ref, here_ref, away_ref, hs_ref, w_ref, s_ref, y_ref, out_ref, mix_ref, *bufs):
    pair_out, pair_in, far_out, far_in, near_out, near_in = bufs[:6]
    pair_left, pair_here, far_left, far_here, near_left, near_here = bufs[6:]
    tokens = pos_ref.shape[0]
    rows = out_ref.shape[2]
    half = tokens // 2
    j = pl.program_id(0)
    partner, beside_y, beside_x = others()
    barrier = pltpu.get_barrier_semaphore()

    def pair(i):
        return remote(pair_out.at[i % 2], pair_in.at[i % 6], pair_left.at[i % 2], pair_here.at[i % 6], partner)

    def far(i, k):
        part = far_out.at[i % 2, k]
        return remote(part, far_in.at[i % 4, k], far_left.at[i % 2, k], far_here.at[i % 4, k], (beside_x, beside_y)[k])

    def near(i, k):
        part = near_out.at[i % 2, k]
        return remote(part, near_in.at[i % 4, k], near_left.at[i % 2, k], near_here.at[i % 4, k], (beside_x, beside_y)[k])

    def term(i, b):
        seen = [out_ref[i % 4, e, b * WIN : (b + 1) * WIN, :] for e in range(own)]
        return dot(mix_ref[b], jnp.concatenate(seen, axis=0))

    @pl.when(j == 0)
    def _():
        lane = lax.broadcasted_iota(jnp.int32, (tokens, WIN), 1)
        for b in range(n):
            for e in range(own):
                i = b * own + e
                hit = pos_ref[:, i : i + 1] == lane
                mix_ref[b, :, e * WIN : (e + 1) * WIN] = jnp.where(hit, gate_ref[:, i : i + 1], 0.0).astype(BF16)
        meet(barrier, (partner, beside_y, beside_x))

    @pl.when(j < tiles)
    def _():
        for e in range(own):
            out_ref[j % 4, e, : 2 * WIN, :] = dot(here_ref[e], w_ref[e]).astype(BF16)
            step = (rows - 2 * WIN) // 2
            for r in (0, step):
                at = 2 * WIN + r
                out_ref[j % 4, e, at : at + step, :] = dot(away_ref[e, r : r + step, :], w_ref[e]).astype(BF16)

        @pl.when(j >= 2)
        def _():
            pair(j - 2).wait_send()

        for q in range(n // 2):
            pair_out[j % 2, q] = term(j, 2 * q + 1).astype(BF16)
        pair(j).start()

    @pl.when((j >= 1) & (j <= tiles))
    def _():
        i = j - 1
        pair(i).wait_recv()

        @pl.when(i >= 2)
        def _():
            far(i - 2, 0).wait_send()
            far(i - 2, 1).wait_send()

        total = (term(i, 6) + pair_in[i % 6, 3].astype(F32)).astype(BF16)
        far_out[i % 2, 0] = total[:half]
        far_out[i % 2, 1] = total[half:]
        far(i, 0).start()
        far(i, 1).start()

    @pl.when((j >= 2) & (j <= tiles + 1))
    def _():
        i = j - 2
        far(i, 0).wait_recv()
        far(i, 1).wait_recv()

        @pl.when(i >= 2)
        def _():
            near(i - 2, 0).wait_send()
            near(i - 2, 1).wait_send()

        total = term(i, 4) + pair_in[i % 6, 2].astype(F32)
        near_out[i % 2, 0, :half] = total[:half].astype(BF16)
        near_out[i % 2, 0, half:] = (total[half:] + far_in[i % 4, 1].astype(F32)).astype(BF16)
        near(i, 0).start()
        total = term(i, 2) + pair_in[i % 6, 1].astype(F32)
        near_out[i % 2, 1, :half] = (total[:half] + far_in[i % 4, 0].astype(F32)).astype(BF16)
        near_out[i % 2, 1, half:] = total[half:].astype(BF16)
        near(i, 1).start()

    @pl.when(j >= 3)
    def _():
        i = j - 3
        total = dot(hs_ref[...], s_ref[...]) + term(i, 0) + pair_in[i % 6, 0].astype(F32)
        near(i, 0).wait_recv()
        near(i, 1).wait_recv()
        total = total + near_in[i % 4, 0].astype(F32) + near_in[i % 4, 1].astype(F32)
        y_ref[...] = total.astype(BF16)

    @pl.when(j == tiles + 2)
    def _():
        for i in (tiles - 2, tiles - 1):
            pair(i).wait_send()
            for k in range(2):
                far(i, k).wait_send()
                near(i, k).wait_send()


def down(here, away, hs, w_down, s_down, pos, gate, tile):
    own, _, ff = here.shape
    n = pos.shape[1] // own
    rows = n * WIN
    tokens, depth = pos.shape[0], w_down.shape[2]
    tiles = depth // tile
    half = tokens // 2
    one = pl.Buffered(1)

    def whole(v):
        return pl.BlockSpec(v.shape, lambda j: (0,) * v.ndim, pipeline_mode=one)

    flops = 2 * own * rows * ff * depth
    dma = pltpu.SemaphoreType.DMA
    return pl.pallas_call(
        functools.partial(down_kernel, n, own, tiles),
        out_shape=jax.ShapeDtypeStruct((tokens, depth), BF16),
        grid=(tiles + 3,),
        in_specs=[
            whole(pos),
            whole(gate),
            whole(here),
            whole(away),
            whole(hs),
            pl.BlockSpec((own, ff, tile), lambda j: (0, 0, jnp.minimum(j, tiles - 1))),
            pl.BlockSpec((s_down.shape[0], tile), lambda j: (0, jnp.maximum(j - 3, 0))),
        ],
        out_specs=pl.BlockSpec((tokens, tile), lambda j: (0, jnp.maximum(j - 3, 0))),
        scratch_shapes=[
            pltpu.VMEM((4, own, rows, tile), BF16),
            pltpu.VMEM((n, tokens, own * WIN), BF16),
            pltpu.VMEM((2, n // 2, tokens, tile), BF16),
            pltpu.VMEM((6, n // 2, tokens, tile), BF16),
            pltpu.VMEM((2, 2, half, tile), BF16),
            pltpu.VMEM((4, 2, half, tile), BF16),
            pltpu.VMEM((2, 2, tokens, tile), BF16),
            pltpu.VMEM((4, 2, tokens, tile), BF16),
            dma((2,)),
            dma((6,)),
            dma((2, 2)),
            dma((4, 2)),
            dma((2, 2)),
            dma((4, 2)),
        ],
        compiler_params=pltpu.CompilerParams(
            vmem_limit_bytes=VMEM_LIMIT, collective_id=0, has_side_effects=True
        ),
        cost_estimate=pl.CostEstimate(flops=flops, bytes_accessed=own * ff * depth * 2, transcendentals=0),
        name="down",
    )(pos, gate, here, away, hs, w_down, s_down)


def solution(mesh):
    n = mesh.shape["ep"]

    def local(x, expert, slot, gate, w_gate, w_up, w_down, s_gate, s_up, s_down):
        me = lax.axis_index("ep")
        x, expert, slot, gate = x[0, 0], expert[0, 0], slot[0, 0], gate[0, 0]
        tokens, top = expert.shape
        own = w_gate.shape[0]
        experts = own * n
        slots = 5 * tokens * top // (4 * experts)

        hit = (expert[:, :, None] == jnp.arange(experts)) & (slot < slots)[:, :, None]
        pos = jnp.sum(jnp.where(hit, slot[:, :, None] + 1, 0), axis=1) - 1
        weight = jnp.sum(jnp.where(hit, gate.astype(BF16).astype(F32)[:, :, None], 0.0), axis=1)
        both = lax.all_gather(jnp.concatenate([pos.astype(F32), weight], axis=1), "ep")
        both = both.reshape(n, tokens, 2, n, own)
        both = lax.dynamic_index_in_dim(both, me, 3, keepdims=False)
        both = both[me ^ jnp.arange(n)]
        pos = both[:, :, 0].astype(jnp.int32)
        weight = both[:, :, 1]
        pos_row = pos.transpose(0, 2, 1).reshape(n * own, tokens)
        pos_col = pos.transpose(1, 0, 2).reshape(tokens, n * own)
        weight = weight.transpose(1, 0, 2).reshape(tokens, n * own)

        hs, here, g, u, far = gather(x, pos_row, s_gate, s_up, w_gate, w_up)
        away = finish(pos_row, far, w_gate, w_up, g, u)
        y = down(here, away, hs, w_down, s_down, pos_col, weight, 512)
        return y[None, None]

    tok, exp, rep = P("dp", "ep"), P("ep"), P()
    return jax.shard_map(
        local,
        mesh=mesh,
        in_specs=(tok, tok, tok, tok, exp, exp, exp, rep, rep, rep),
        out_specs=tok,
        check_vma=False,
    )
```

```python
import functools

import jax
import jax.numpy as jnp
from jax import lax
from jax.experimental import pallas as pl
from jax.experimental.pallas import tpu as pltpu
from jax.sharding import PartitionSpec as P

F32, BF16 = jnp.float32, jnp.bfloat16
VMEM_LIMIT = 62 * 2**20
WIN = 112
TILE = 512
RING = 3


def dot(a, b):
    return lax.dot_general(a, b, (((a.ndim - 1,), (b.ndim - 2,)), ((), ())), preferred_element_type=F32)


def remote(src, dst, left, here, device):
    return pltpu.make_async_remote_copy(
        src_ref=src,
        dst_ref=dst,
        send_sem=left,
        recv_sem=here,
        device_id={"ep": device},
        device_id_type=pl.DeviceIdType.MESH,
    )


def others():
    me = lax.axis_index("ep")
    return me + 1 - 2 * (me % 2), me + 2 - 4 * ((me // 2) % 2), me + 4 - 8 * ((me // 4) % 2)


def flip(index, bits):
    for bit in (1, 2, 4):
        if bits & bit:
            index = index + bit - 2 * bit * ((index // bit) % 2)
    return index


def meet(barrier, devices):
    for device in devices:
        pl.semaphore_signal(barrier, inc=1, device_id={"ep": device}, device_id_type=pl.DeviceIdType.MESH)
    pl.semaphore_wait(barrier, len(devices))


def up_kernel(own, n, plan, note_ref, x_ref, sg_ref, su_ref, wg_ref, wu_ref, *refs):
    hs_ref, here_ref, away_ref, out_ref, far_ref, acc_ref = refs[:6]
    ring_ref, notes_ref, xp_ref, xr_ref, zp_ref, zr_ref, ga_ref, ua_ref, wide_ref = refs[6:15]
    note_left, note_here, pair_left, pair_here, left, here, ring_sem, load_sem, acc_sem = refs[15:]
    shared, pairs, rest, per = plan
    t = pl.program_id(0)
    depth = ring_ref.shape[2]
    half = x_ref.shape[0] // 2
    me = lax.axis_index("ep")
    partner, beside_y, beside_x = others()
    barrier = pltpu.get_barrier_semaphore()
    late = shared + pairs

    def block(c, q):
        return xr_ref.at[q] if c == 0 else far_ref.at[q]

    def copy(c, k):
        if k < 2:
            src, dst, device = x_ref.at[:, pl.ds(c * depth, depth)], block(c, 2 * k), (beside_y, beside_x)[k]
        elif k == 2:
            src, dst, device = block(c, 2).at[pl.ds(0, half)], block(c, 4).at[pl.ds(0, half)], beside_y
        elif k == 3:
            src, dst, device = block(c, 0).at[pl.ds(half, half)], block(c, 4).at[pl.ds(half, half)], beside_x
        else:
            src, dst, device = block(c, 2 * k - 8), block(c, 2 * k - 7), partner
        return remote(src, dst, left.at[c, k], here.at[c, k], device)

    pair = remote(x_ref, xp_ref, pair_left.at[0], pair_here.at[0], partner)

    def note(b):
        device = flip(me, b)
        return remote(note_ref.at[device], notes_ref.at[b], note_left.at[b], note_here.at[b], device)

    def weights(s, src, k, g):
        slot = s % RING
        return pltpu.make_async_copy(src, ring_ref.at[slot, g], ring_sem.at[slot, g])

    def fetch(s):
        @pl.when(s < shared)
        def _():
            at = pl.ds((s % 2) * depth, depth), pl.ds((s // 2) * TILE, TILE)
            for g, ref in enumerate((sg_ref, su_ref)):
                weights(s, ref.at[at], s % 2, g).start()

        @pl.when((s >= shared) & (s < late))
        def _():
            p = s - shared
            at = p // (2 * per), pl.ds((p % 2) * depth, depth), pl.ds((p // 2 % per) * TILE, TILE)
            for g, ref in enumerate((wg_ref, wu_ref)):
                weights(s, ref.at[at], p % 2, g).start()

        @pl.when((s >= late) & (s < late + 2 * rest))
        def _():
            r = (s - late) % rest
            k = (s - late) // rest
            at = r // per, pl.ds(k * depth, depth), pl.ds((r % per) * TILE, TILE)
            for g, ref in enumerate((wg_ref, wu_ref)):
                weights(s, ref.at[at], k, g).start()

    def load(q):
        return pltpu.make_async_copy(far_ref.at[q], xr_ref.at[q], load_sem.at[q])

    def spill(r):
        return pltpu.make_async_copy(wide_ref.at[r % 2], acc_ref.at[r], acc_sem.at[r % 2])

    def refill(r):
        return pltpu.make_async_copy(acc_ref.at[r], wide_ref.at[r % 2], acc_sem.at[r % 2])

    @pl.when(t == 0)
    def _():
        for s in range(RING):
            fetch(s)
        notes_ref[0] = note_ref[me]
        meet(barrier, [flip(me, b) for b in range(1, n)])
        for b in range(1, n):
            note(b).start()
        copy(0, 0).start()
        copy(0, 1).start()
        pair.start()

    def forward(c):
        copy(c, 0).wait_recv()
        copy(c, 1).wait_recv()
        for k in (2, 3, 4, 5):
            copy(c, k).start()

    def onward(c):
        copy(c, 2).wait_recv()
        copy(c, 3).wait_recv()
        copy(c, 6).start()

    def arrived(c):
        for k in (4, 5, 6):
            copy(c, k).wait_recv()

    @pl.when(t == shared + 10)
    def _():
        forward(0)
        copy(1, 0).start()
        copy(1, 1).start()

    @pl.when(t == shared + 20)
    def _():
        onward(0)

    @pl.when(t == late + 6)
    def _():
        forward(1)

    @pl.when(t == late + 10)
    def _():
        onward(1)

    @pl.when(t == late + rest - 1)
    def _():
        arrived(1)
        for k in range(2, 7):
            copy(0, k).wait_send()
        for q in range(n - 2):
            load(q).start()

    for g in range(2):
        weights(t, wg_ref.at[0, pl.ds(0, depth), pl.ds(0, TILE)], 0, g).wait()
    wg, wu = ring_ref.at[t % RING, 0], ring_ref.at[t % RING, 1]

    def two_halves(k, z_ref, rows, store):
        for part in range(2):

            @pl.when(k == part)
            def _():
                z = z_ref[:rows, part * depth : (part + 1) * depth]
                g, u = dot(z, wg[...]), dot(z, wu[...])
                if part == 0:
                    ga_ref[:rows] = g
                    ua_ref[:rows] = u
                else:
                    g, u = g + ga_ref[:rows], u + ua_ref[:rows]
                    store((jax.nn.silu(g) * u).astype(BF16))

    @pl.when(t < shared)
    def _():
        def store(v):
            hs_ref[...] = v

        two_halves(t % 2, x_ref, x_ref.shape[0], store)

    @pl.when((t >= shared) & (t < late))
    def _():
        p = t - shared

        @pl.when(p == 0)
        def _():
            pair.wait_recv()
            note(1).wait_recv()

        @pl.when(p % (2 * per) == 0)
        def _():
            e = p // (2 * per)
            dispatch(notes_ref, 0, e, x_ref, zp_ref, 0)
            dispatch(notes_ref, 1, e, xp_ref, zp_ref, WIN)

        def store(v):
            here_ref[0] = v

        two_halves(p % 2, zp_ref, 2 * WIN, store)

    @pl.when(t >= late)
    def _():
        r = (t - late) % rest
        k = (t - late) // rest

        @pl.when(t == late)
        def _():
            arrived(0)
            for b in range(2, n):
                note(b).wait_recv()
            out_ref[...] = notes_ref[...]

        @pl.when(t == late + rest)
        def _():
            for q in range(n - 2):
                load(q).wait()
            for i in (rest - 2, rest - 1):
                spill(i).wait()
            for i in (0, 1):
                refill(i).start()

        @pl.when(r % per == 0)
        def _():
            for q in range(n - 2):
                dispatch(notes_ref, q + 2, r // per, xr_ref.at[q], zr_ref, q * WIN)

        rows = zr_ref.shape[0] // 2

        @pl.when(k == 0)
        def _():
            @pl.when(r >= 2)
            def _():
                spill(r - 2).wait()

            for m in (0, rows):
                z = zr_ref[m : m + rows, :]
                wide_ref[r % 2, 0, m : m + rows, :] = dot(z, wg[...])
                wide_ref[r % 2, 1, m : m + rows, :] = dot(z, wu[...])
            spill(r).start()

        @pl.when(k == 1)
        def _():
            refill(r).wait()
            for m in (0, rows):
                z = zr_ref[m : m + rows, :]
                g = dot(z, wg[...]) + wide_ref[r % 2, 0, m : m + rows, :]
                u = dot(z, wu[...]) + wide_ref[r % 2, 1, m : m + rows, :]
                away_ref[0, m : m + rows, :] = (jax.nn.silu(g) * u).astype(BF16)

            @pl.when(r < rest - 2)
            def _():
                refill(r + 2).start()

    fetch(t + RING)

    @pl.when(t == late + 2 * rest - 1)
    def _():
        pair.wait_send()
        for b in range(1, n):
            note(b).wait_send()
        for k in range(7):
            if k < 2:
                copy(0, k).wait_send()
            copy(1, k).wait_send()


def dispatch(notes_ref, b, e, x_ref, z_ref, at):
    pos = notes_ref[b, pl.ds(e, 1), :]
    slot = lax.broadcasted_iota(jnp.int32, (WIN, pos.shape[1]), 0).astype(F32)
    hot = (slot == pos).astype(F32).astype(BF16)
    for k in range(0, z_ref.shape[1], 512):
        z_ref[at : at + WIN, k : k + 512] = dot(hot, x_ref[:, k : k + 512]).astype(BF16)


def up(x, note, s_gate, s_up, w_gate, w_up):
    tokens, depth = x.shape
    own, _, ff = w_gate.shape
    n = note.shape[0]
    half = depth // 2
    per = ff // TILE
    shared, pairs, rest = 2 * s_gate.shape[1] // TILE, 2 * own * per, own * per
    late = shared + pairs
    rows = (n - 2) * WIN
    one = pl.Buffered(1)

    def whole(v):
        return pl.BlockSpec(v.shape, lambda t: (0,) * v.ndim, pipeline_mode=one)

    def here_at(t):
        p = jnp.clip(t - shared, 0, pairs - 1)
        return p // (2 * per), 0, p // 2 % per

    def away_at(t):
        r = jnp.maximum(t - late - rest, 0)
        return r // per, 0, r % per

    anywhere = pl.BlockSpec(memory_space=pl.ANY)
    dma = pltpu.SemaphoreType.DMA
    flops = 4 * (tokens * s_gate.shape[1] + own * (2 * WIN + rows) * ff) * depth
    return pl.pallas_call(
        functools.partial(up_kernel, own, n, (shared, pairs, rest, per)),
        out_shape=(
            jax.ShapeDtypeStruct((tokens, s_gate.shape[1]), BF16),
            jax.ShapeDtypeStruct((own, 2 * WIN, ff), BF16),
            jax.ShapeDtypeStruct((own, rows, ff), BF16),
            jax.ShapeDtypeStruct(note.shape, F32),
            jax.ShapeDtypeStruct((n - 2, tokens, half), BF16),
            jax.ShapeDtypeStruct((rest, 2, rows, TILE), F32),
        ),
        grid=(late + 2 * rest,),
        in_specs=[whole(note), whole(x)] + [anywhere] * 4,
        out_specs=(
            pl.BlockSpec((tokens, TILE), lambda t: (0, jnp.minimum(t, shared - 1) // 2)),
            pl.BlockSpec((1, 2 * WIN, TILE), here_at),
            pl.BlockSpec((1, rows, TILE), away_at),
            whole(note),
            anywhere,
            anywhere,
        ),
        scratch_shapes=[
            pltpu.VMEM((RING, 2, half, TILE), BF16),
            pltpu.VMEM(note.shape, F32),
            pltpu.VMEM((tokens, depth), BF16),
            pltpu.VMEM((n - 2, tokens, half), BF16),
            pltpu.VMEM((2 * WIN, depth), BF16),
            pltpu.VMEM((rows, half), BF16),
            pltpu.VMEM((tokens, TILE), F32),
            pltpu.VMEM((tokens, TILE), F32),
            pltpu.VMEM((2, 2, rows, TILE), F32),
            dma((n,)),
            dma((n,)),
            dma((1,)),
            dma((1,)),
            dma((2, 7)),
            dma((2, 7)),
            dma((RING, 2)),
            dma((n - 2,)),
            dma((2,)),
        ],
        compiler_params=pltpu.CompilerParams(
            vmem_limit_bytes=VMEM_LIMIT, collective_id=1, has_side_effects=True
        ),
        cost_estimate=pl.CostEstimate(flops=flops, bytes_accessed=own * 4 * depth * ff * 2, transcendentals=0),
        name="up",
    )(note, x, s_gate, s_up, w_gate, w_up)[:4]


def down_kernel(n, own, tiles, pos_ref, gate_ref, here_ref, away_ref, hs_ref, w_ref, s_ref, y_ref, out_ref, mix_ref, *bufs):
    pair_out, pair_in, far_out, far_in, near_out, near_in = bufs[:6]
    pair_left, pair_here, far_left, far_here, near_left, near_here = bufs[6:]
    tokens = pos_ref.shape[0]
    rows = out_ref.shape[2]
    half = tokens // 2
    j = pl.program_id(0)
    partner, beside_y, beside_x = others()
    barrier = pltpu.get_barrier_semaphore()

    def pair(i):
        return remote(pair_out.at[i % 2], pair_in.at[i % 6], pair_left.at[i % 2], pair_here.at[i % 6], partner)

    def far(i, k):
        part = far_out.at[i % 2, k]
        return remote(part, far_in.at[i % 4, k], far_left.at[i % 2, k], far_here.at[i % 4, k], (beside_x, beside_y)[k])

    def near(i, k):
        part = near_out.at[i % 2, k]
        return remote(part, near_in.at[i % 4, k], near_left.at[i % 2, k], near_here.at[i % 4, k], (beside_x, beside_y)[k])

    def term(i, b):
        seen = [out_ref[i % 4, e, b * WIN : (b + 1) * WIN, :] for e in range(own)]
        return dot(mix_ref[b], jnp.concatenate(seen, axis=0))

    @pl.when(j == 0)
    def _():
        lane = lax.broadcasted_iota(jnp.int32, (tokens, WIN), 1)
        for b in range(n):
            for e in range(own):
                i = b * own + e
                hit = pos_ref[:, i : i + 1] == lane
                mix_ref[b, :, e * WIN : (e + 1) * WIN] = jnp.where(hit, gate_ref[:, i : i + 1], 0.0).astype(BF16)
        meet(barrier, (partner, beside_y, beside_x))

    def project(e):
        out_ref[j % 4, e, : 2 * WIN, :] = dot(here_ref[e], w_ref[e]).astype(BF16)
        step = (rows - 2 * WIN) // 2
        for r in (0, step):
            at = 2 * WIN + r
            out_ref[j % 4, e, at : at + step, :] = dot(away_ref[e, r : r + step, :], w_ref[e]).astype(BF16)

    @pl.when(j < tiles)
    def _():
        for e in range(3):
            project(e)

    @pl.when((j >= 1) & (j <= tiles))
    def _():
        i = j - 1
        pair(i).wait_recv()

        @pl.when(i >= 2)
        def _():
            far(i - 2, 0).wait_send()
            far(i - 2, 1).wait_send()

        total = (term(i, 6) + pair_in[i % 6, 3].astype(F32)).astype(BF16)
        far_out[i % 2, 0] = total[:half]
        far_out[i % 2, 1] = total[half:]
        far(i, 0).start()
        far(i, 1).start()

    @pl.when((j >= 2) & (j <= tiles + 1))
    def _():
        i = j - 2
        far(i, 0).wait_recv()
        far(i, 1).wait_recv()

        @pl.when(i >= 2)
        def _():
            near(i - 2, 0).wait_send()
            near(i - 2, 1).wait_send()

        total = term(i, 4) + pair_in[i % 6, 2].astype(F32)
        near_out[i % 2, 0, :half] = total[:half].astype(BF16)
        near_out[i % 2, 0, half:] = (total[half:] + far_in[i % 4, 1].astype(F32)).astype(BF16)
        near(i, 0).start()
        total = term(i, 2) + pair_in[i % 6, 1].astype(F32)
        near_out[i % 2, 1, :half] = (total[:half] + far_in[i % 4, 0].astype(F32)).astype(BF16)
        near_out[i % 2, 1, half:] = total[half:].astype(BF16)
        near(i, 1).start()

    @pl.when(j >= 3)
    def _():
        i = j - 3
        total = dot(hs_ref[...], s_ref[...]) + term(i, 0) + pair_in[i % 6, 0].astype(F32)
        near(i, 0).wait_recv()
        near(i, 1).wait_recv()
        total = total + near_in[i % 4, 0].astype(F32) + near_in[i % 4, 1].astype(F32)
        y_ref[...] = total.astype(BF16)

    @pl.when(j < tiles)
    def _():
        for e in range(3, own):
            project(e)

        @pl.when(j >= 2)
        def _():
            pair(j - 2).wait_send()

        for q in range(n // 2):
            pair_out[j % 2, q] = term(j, 2 * q + 1).astype(BF16)
        pair(j).start()

    @pl.when(j == tiles + 2)
    def _():
        for i in (tiles - 2, tiles - 1):
            pair(i).wait_send()
            for k in range(2):
                far(i, k).wait_send()
                near(i, k).wait_send()


def down(here, away, hs, w_down, s_down, pos, gate, tile):
    own, _, ff = here.shape
    n = pos.shape[1] // own
    rows = n * WIN
    tokens, depth = pos.shape[0], w_down.shape[2]
    tiles = depth // tile
    half = tokens // 2
    one = pl.Buffered(1)

    def whole(v):
        return pl.BlockSpec(v.shape, lambda j: (0,) * v.ndim, pipeline_mode=one)

    flops = 2 * own * rows * ff * depth
    dma = pltpu.SemaphoreType.DMA
    return pl.pallas_call(
        functools.partial(down_kernel, n, own, tiles),
        out_shape=jax.ShapeDtypeStruct((tokens, depth), BF16),
        grid=(tiles + 3,),
        in_specs=[
            whole(pos),
            whole(gate),
            whole(here),
            whole(away),
            whole(hs),
            pl.BlockSpec((own, ff, tile), lambda j: (0, 0, jnp.minimum(j, tiles - 1))),
            pl.BlockSpec((s_down.shape[0], tile), lambda j: (0, jnp.maximum(j - 3, 0))),
        ],
        out_specs=pl.BlockSpec((tokens, tile), lambda j: (0, jnp.maximum(j - 3, 0))),
        scratch_shapes=[
            pltpu.VMEM((4, own, rows, tile), BF16),
            pltpu.VMEM((n, tokens, own * WIN), BF16),
            pltpu.VMEM((2, n // 2, tokens, tile), BF16),
            pltpu.VMEM((6, n // 2, tokens, tile), BF16),
            pltpu.VMEM((2, 2, half, tile), BF16),
            pltpu.VMEM((4, 2, half, tile), BF16),
            pltpu.VMEM((2, 2, tokens, tile), BF16),
            pltpu.VMEM((4, 2, tokens, tile), BF16),
            dma((2,)),
            dma((6,)),
            dma((2, 2)),
            dma((4, 2)),
            dma((2, 2)),
            dma((4, 2)),
        ],
        compiler_params=pltpu.CompilerParams(
            vmem_limit_bytes=VMEM_LIMIT, collective_id=0, has_side_effects=True
        ),
        cost_estimate=pl.CostEstimate(flops=flops, bytes_accessed=own * ff * depth * 2, transcendentals=0),
        name="down",
    )(pos, gate, here, away, hs, w_down, s_down)


def solution(mesh):
    n = mesh.shape["ep"]

    def local(x, expert, slot, gate, w_gate, w_up, w_down, s_gate, s_up, s_down):
        x, expert, slot, gate = x[0, 0], expert[0, 0], slot[0, 0], gate[0, 0]
        tokens, top = expert.shape
        own = w_gate.shape[0]
        experts = own * n
        slots = 5 * tokens * top // (4 * experts)

        hit = (expert[:, :, None] == jnp.arange(experts)) & (slot < slots)[:, :, None]
        pos = jnp.sum(jnp.where(hit, slot[:, :, None] + 1, 0), axis=1) - 1
        weight = jnp.sum(jnp.where(hit, gate.astype(BF16).astype(F32)[:, :, None], 0.0), axis=1)
        note = jnp.stack([pos.astype(F32), weight]).reshape(2, tokens, n, own).transpose(2, 0, 3, 1)
        note = jnp.pad(note.reshape(n, 2 * own, tokens), ((0, 0), (0, 8 - 2 * own), (0, 0)))
        hs, here, away, notes = up(x, note, s_gate, s_up, w_gate, w_up)
        pos_col = notes[:, :own].reshape(n * own, tokens).T.astype(jnp.int32)
        weight = notes[:, own : 2 * own].reshape(n * own, tokens).T
        y = down(here, away, hs, w_down, s_down, pos_col, weight, 512)
        return y[None, None]

    tok, exp, rep = P("dp", "ep"), P("ep"), P()
    return jax.shard_map(
        local,
        mesh=mesh,
        in_specs=(tok, tok, tok, tok, exp, exp, exp, rep, rep, rep),
        out_specs=tok,
        check_vma=False,
    )
```

```python
import functools

import jax
import jax.numpy as jnp
from jax import lax
from jax.experimental import pallas as pl
from jax.experimental.pallas import tpu as pltpu
from jax.sharding import PartitionSpec as P

F32, BF16 = jnp.float32, jnp.bfloat16
VMEM_LIMIT = 62 * 2**20
WIN = 112
TILE = 512
RING = 3


def dot(a, b):
    return lax.dot_general(a, b, (((a.ndim - 1,), (b.ndim - 2,)), ((), ())), preferred_element_type=F32)


def window(q, slots):
    first = q * slots // 16 * 16
    shift = q * slots - first
    return first, shift, (shift + slots + 15) // 16 * 16


def remote(src, dst, left, here, device):
    return pltpu.make_async_remote_copy(
        src_ref=src,
        dst_ref=dst,
        send_sem=left,
        recv_sem=here,
        device_id={"ep": device},
        device_id_type=pl.DeviceIdType.MESH,
    )


def others():
    me = lax.axis_index("ep")
    return me + 1 - 2 * (me % 2), me + 2 - 4 * ((me // 2) % 2), me + 4 - 8 * ((me // 4) % 2)


def flip(index, bits):
    for bit in (1, 2, 4):
        if bits & bit:
            index = index + bit - 2 * bit * ((index // bit) % 2)
    return index


def meet(barrier, devices):
    for device in devices:
        pl.semaphore_signal(barrier, inc=1, device_id={"ep": device}, device_id_type=pl.DeviceIdType.MESH)
    pl.semaphore_wait(barrier, len(devices))


def up_kernel(own, n, slots, plan, note_ref, x_ref, sg_ref, su_ref, wg_ref, wu_ref, *refs):
    hs_ref, here_ref, away_ref, out_ref, far_ref, acc_ref = refs[:6]
    ring_ref, notes_ref, xp_ref, xr_ref, zp_ref, zr_ref, ga_ref, ua_ref, wide_ref = refs[6:15]
    note_left, note_here, pair_left, pair_here, left, here, ring_sem, load_sem, acc_sem = refs[15:]
    shared, pairs, rest, per = plan
    t = pl.program_id(0)
    depth = ring_ref.shape[2]
    half = x_ref.shape[0] // 2
    me = lax.axis_index("ep")
    partner, beside_y, beside_x = others()
    barrier = pltpu.get_barrier_semaphore()
    late = shared + pairs

    def block(c, q):
        return xr_ref.at[q] if c == 0 else far_ref.at[q]

    def copy(c, k):
        if k < 2:
            src, dst, device = x_ref.at[:, pl.ds(c * depth, depth)], block(c, 2 * k), (beside_y, beside_x)[k]
        elif k == 2:
            src, dst, device = block(c, 2).at[pl.ds(0, half)], block(c, 4).at[pl.ds(0, half)], beside_y
        elif k == 3:
            src, dst, device = block(c, 0).at[pl.ds(half, half)], block(c, 4).at[pl.ds(half, half)], beside_x
        else:
            src, dst, device = block(c, 2 * k - 8), block(c, 2 * k - 7), partner
        return remote(src, dst, left.at[c, k], here.at[c, k], device)

    pair = remote(x_ref, xp_ref, pair_left.at[0], pair_here.at[0], partner)

    def note(b):
        device = flip(me, b)
        return remote(note_ref.at[device], notes_ref.at[b], note_left.at[b], note_here.at[b], device)

    def weights(s, src, k, g):
        slot = s % RING
        return pltpu.make_async_copy(src, ring_ref.at[slot, g], ring_sem.at[slot, g])

    def fetch(s):
        @pl.when(s < shared)
        def _():
            at = pl.ds((s % 2) * depth, depth), pl.ds((s // 2) * TILE, TILE)
            for g, ref in enumerate((sg_ref, su_ref)):
                weights(s, ref.at[at], s % 2, g).start()

        @pl.when((s >= shared) & (s < late))
        def _():
            p = s - shared
            at = p // (2 * per), pl.ds((p % 2) * depth, depth), pl.ds((p // 2 % per) * TILE, TILE)
            for g, ref in enumerate((wg_ref, wu_ref)):
                weights(s, ref.at[at], p % 2, g).start()

        @pl.when((s >= late) & (s < late + 2 * rest))
        def _():
            r = (s - late) % rest
            k = (s - late) // rest
            at = r // per, pl.ds(k * depth, depth), pl.ds((r % per) * TILE, TILE)
            for g, ref in enumerate((wg_ref, wu_ref)):
                weights(s, ref.at[at], k, g).start()

    def load(q):
        return pltpu.make_async_copy(far_ref.at[q], xr_ref.at[q], load_sem.at[q])

    def spill(r):
        return pltpu.make_async_copy(wide_ref.at[r % 2], acc_ref.at[r], acc_sem.at[r % 2])

    def refill(r):
        return pltpu.make_async_copy(acc_ref.at[r], wide_ref.at[r % 2], acc_sem.at[r % 2])

    @pl.when(t == 0)
    def _():
        for s in range(RING):
            fetch(s)
        notes_ref[0] = note_ref[me]
        meet(barrier, [flip(me, b) for b in range(1, n)])
        for b in range(1, n):
            note(b).start()
        copy(0, 0).start()
        copy(0, 1).start()
        pair.start()

    def forward(c):
        copy(c, 0).wait_recv()
        copy(c, 1).wait_recv()
        for k in (2, 3, 4, 5):
            copy(c, k).start()

    def onward(c):
        copy(c, 2).wait_recv()
        copy(c, 3).wait_recv()
        copy(c, 6).start()

    def arrived(c):
        for k in (4, 5, 6):
            copy(c, k).wait_recv()

    @pl.when(t == shared + 10)
    def _():
        forward(0)
        copy(1, 0).start()
        copy(1, 1).start()

    @pl.when(t == shared + 20)
    def _():
        onward(0)

    @pl.when(t == late + 6)
    def _():
        forward(1)

    @pl.when(t == late + 10)
    def _():
        onward(1)

    @pl.when(t == late + rest - 1)
    def _():
        arrived(1)
        for k in range(2, 7):
            copy(0, k).wait_send()
        for q in range(n - 2):
            load(q).start()

    for g in range(2):
        weights(t, wg_ref.at[0, pl.ds(0, depth), pl.ds(0, TILE)], 0, g).wait()
    wg, wu = ring_ref.at[t % RING, 0], ring_ref.at[t % RING, 1]

    def two_halves(k, z_ref, rows, store):
        for part in range(2):

            @pl.when(k == part)
            def _():
                z = z_ref[:rows, part * depth : (part + 1) * depth]
                g, u = dot(z, wg[...]), dot(z, wu[...])
                if part == 0:
                    ga_ref[:rows] = g
                    ua_ref[:rows] = u
                else:
                    g, u = g + ga_ref[:rows], u + ua_ref[:rows]
                    store((jax.nn.silu(g) * u).astype(BF16))

    @pl.when(t < shared)
    def _():
        def store(v):
            hs_ref[...] = v

        two_halves(t % 2, x_ref, x_ref.shape[0], store)

    @pl.when((t >= shared) & (t < late))
    def _():
        p = t - shared

        @pl.when(p == 0)
        def _():
            pair.wait_recv()
            note(1).wait_recv()

        @pl.when(p % (2 * per) == 0)
        def _():
            e = p // (2 * per)
            dispatch(notes_ref, 0, e, x_ref, zp_ref, (0, 0, WIN))
            dispatch(notes_ref, 1, e, xp_ref, zp_ref, (WIN, 0, WIN))

        def store(v):
            here_ref[0] = v

        two_halves(p % 2, zp_ref, 2 * WIN, store)

    @pl.when(t >= late)
    def _():
        r = (t - late) % rest
        k = (t - late) // rest

        @pl.when(t == late)
        def _():
            arrived(0)
            for b in range(2, n):
                note(b).wait_recv()
            out_ref[...] = notes_ref[...]

        @pl.when(t == late + rest)
        def _():
            for q in range(n - 2):
                load(q).wait()
            for i in (rest - 2, rest - 1):
                spill(i).wait()
            for i in (0, 1):
                refill(i).start()

        @pl.when(r % per == 0)
        def _():
            for q in range(n - 2):
                dispatch(notes_ref, q + 2, r // per, xr_ref.at[q], zr_ref, window(q, slots))

        rows = zr_ref.shape[0] // 2

        @pl.when(k == 0)
        def _():
            @pl.when(r >= 2)
            def _():
                spill(r - 2).wait()

            for m in (0, rows):
                z = zr_ref[m : m + rows, :]
                wide_ref[r % 2, 0, m : m + rows, :] = dot(z, wg[...])
                wide_ref[r % 2, 1, m : m + rows, :] = dot(z, wu[...])
            spill(r).start()

        @pl.when(k == 1)
        def _():
            refill(r).wait()
            for m in (0, rows):
                z = zr_ref[m : m + rows, :]
                g = dot(z, wg[...]) + wide_ref[r % 2, 0, m : m + rows, :]
                u = dot(z, wu[...]) + wide_ref[r % 2, 1, m : m + rows, :]
                away_ref[0, m : m + rows, :] = (jax.nn.silu(g) * u).astype(BF16)

            @pl.when(r < rest - 2)
            def _():
                refill(r + 2).start()

    fetch(t + RING)

    @pl.when(t == late + 2 * rest - 1)
    def _():
        pair.wait_send()
        for b in range(1, n):
            note(b).wait_send()
        for k in range(7):
            if k < 2:
                copy(0, k).wait_send()
            copy(1, k).wait_send()


def dispatch(notes_ref, b, e, x_ref, z_ref, at):
    first, shift, rows = at
    pos = notes_ref[b, pl.ds(e, 1), :]
    pos = jnp.where(pos < 0, -1.0, pos + shift)
    row = lax.broadcasted_iota(jnp.int32, (rows, pos.shape[1]), 0).astype(F32)
    hot = (row == pos).astype(F32).astype(BF16)
    for k in range(0, z_ref.shape[1], 512):
        cols = slice(k, k + 512)
        got = dot(hot, x_ref[:, cols])
        if shift:
            z_ref[first : first + 16, cols] = (got[:16] + z_ref[first : first + 16, cols].astype(F32)).astype(BF16)
            z_ref[first + 16 : first + rows, cols] = got[16:].astype(BF16)
        else:
            z_ref[first : first + rows, cols] = got.astype(BF16)


def up(x, note, slots, s_gate, s_up, w_gate, w_up):
    tokens, depth = x.shape
    own, _, ff = w_gate.shape
    n = note.shape[0]
    half = depth // 2
    per = ff // TILE
    shared, pairs, rest = 2 * s_gate.shape[1] // TILE, 2 * own * per, own * per
    late = shared + pairs
    rows = (n - 2) * slots
    rows = (rows + 31) // 32 * 32
    one = pl.Buffered(1)

    def whole(v):
        return pl.BlockSpec(v.shape, lambda t: (0,) * v.ndim, pipeline_mode=one)

    def here_at(t):
        p = jnp.clip(t - shared, 0, pairs - 1)
        return p // (2 * per), 0, p // 2 % per

    def away_at(t):
        r = jnp.maximum(t - late - rest, 0)
        return r // per, 0, r % per

    anywhere = pl.BlockSpec(memory_space=pl.ANY)
    dma = pltpu.SemaphoreType.DMA
    flops = 4 * (tokens * s_gate.shape[1] + own * (2 * WIN + rows) * ff) * depth
    return pl.pallas_call(
        functools.partial(up_kernel, own, n, slots, (shared, pairs, rest, per)),
        out_shape=(
            jax.ShapeDtypeStruct((tokens, s_gate.shape[1]), BF16),
            jax.ShapeDtypeStruct((own, 2 * WIN, ff), BF16),
            jax.ShapeDtypeStruct((own, rows, ff), BF16),
            jax.ShapeDtypeStruct(note.shape, F32),
            jax.ShapeDtypeStruct((n - 2, tokens, half), BF16),
            jax.ShapeDtypeStruct((rest, 2, rows, TILE), F32),
        ),
        grid=(late + 2 * rest,),
        in_specs=[whole(note), whole(x)] + [anywhere] * 4,
        out_specs=(
            pl.BlockSpec((tokens, TILE), lambda t: (0, jnp.minimum(t, shared - 1) // 2)),
            pl.BlockSpec((1, 2 * WIN, TILE), here_at),
            pl.BlockSpec((1, rows, TILE), away_at),
            whole(note),
            anywhere,
            anywhere,
        ),
        scratch_shapes=[
            pltpu.VMEM((RING, 2, half, TILE), BF16),
            pltpu.VMEM(note.shape, F32),
            pltpu.VMEM((tokens, depth), BF16),
            pltpu.VMEM((n - 2, tokens, half), BF16),
            pltpu.VMEM((2 * WIN, depth), BF16),
            pltpu.VMEM((rows, half), BF16),
            pltpu.VMEM((tokens, TILE), F32),
            pltpu.VMEM((tokens, TILE), F32),
            pltpu.VMEM((2, 2, rows, TILE), F32),
            dma((n,)),
            dma((n,)),
            dma((1,)),
            dma((1,)),
            dma((2, 7)),
            dma((2, 7)),
            dma((RING, 2)),
            dma((n - 2,)),
            dma((2,)),
        ],
        compiler_params=pltpu.CompilerParams(
            vmem_limit_bytes=VMEM_LIMIT, collective_id=1, has_side_effects=True
        ),
        cost_estimate=pl.CostEstimate(flops=flops, bytes_accessed=own * 4 * depth * ff * 2, transcendentals=0),
        name="up",
    )(note, x, s_gate, s_up, w_gate, w_up)[:4]


def down_kernel(n, own, slots, tiles, pos_ref, gate_ref, here_ref, away_ref, hs_ref, w_ref, s_ref, y_ref, h_ref, out_ref, mix_ref, *bufs):
    pair_out, pair_in, far_out, far_in, near_out, near_in = bufs[:6]
    pair_left, pair_here, far_left, far_here, near_left, near_here, h_sem = bufs[6:]
    tokens = pos_ref.shape[0]
    rows = out_ref.shape[2]
    half = tokens // 2
    j = pl.program_id(0)
    partner, beside_y, beside_x = others()
    barrier = pltpu.get_barrier_semaphore()

    def pair(i):
        return remote(pair_out.at[i % 2], pair_in.at[i % 6], pair_left.at[i % 2], pair_here.at[i % 6], partner)

    def far(i, k):
        part = far_out.at[i % 2, k]
        return remote(part, far_in.at[i % 4, k], far_left.at[i % 2, k], far_here.at[i % 4, k], (beside_x, beside_y)[k])

    def near(i, k):
        part = near_out.at[i % 2, k]
        return remote(part, near_in.at[i % 4, k], near_left.at[i % 2, k], near_here.at[i % 4, k], (beside_x, beside_y)[k])

    def term(i, b):
        first, _, size = seat(b)
        seen = [out_ref[i % 4, e, first : first + size, :] for e in range(own)]
        return dot(mix_ref[b, :, : own * size], jnp.concatenate(seen, axis=0))

    def seat(b):
        if b < 2:
            return b * WIN, 0, WIN
        first, shift, size = window(b - 2, slots)
        return 2 * WIN + first, shift, size

    def parts(e):
        return (
            pltpu.make_async_copy(here_ref.at[e], h_ref.at[e, pl.ds(0, 2 * WIN)], h_sem.at[e, 0]),
            pltpu.make_async_copy(away_ref.at[e], h_ref.at[e, pl.ds(2 * WIN, rows - 2 * WIN)], h_sem.at[e, 1]),
        )

    @pl.when(j == 0)
    def _():
        for e in range(own):
            for part in parts(e):
                part.start()
        for b in range(n):
            _, shift, size = seat(b)
            lane = lax.broadcasted_iota(jnp.int32, (tokens, size), 1)
            for e in range(own):
                i = b * own + e
                pos = pos_ref[:, i : i + 1]
                hit = jnp.where(pos < 0, -1, pos + shift) == lane
                mix_ref[b, :, e * size : (e + 1) * size] = jnp.where(hit, gate_ref[:, i : i + 1], 0.0).astype(BF16)
        meet(barrier, (partner, beside_y, beside_x))

    def project(e):
        @pl.when(j == 0)
        def _():
            for part in parts(e):
                part.wait()

        step = rows // 2
        for r in (0, step):
            out_ref[j % 4, e, r : r + step, :] = dot(h_ref[e, r : r + step, :], w_ref[e]).astype(BF16)

    @pl.when(j < tiles)
    def _():
        for e in range(3):
            project(e)

    @pl.when((j >= 1) & (j <= tiles))
    def _():
        i = j - 1
        pair(i).wait_recv()

        @pl.when(i >= 2)
        def _():
            far(i - 2, 0).wait_send()
            far(i - 2, 1).wait_send()

        total = (term(i, 6) + pair_in[i % 6, 3].astype(F32)).astype(BF16)
        far_out[i % 2, 0] = total[:half]
        far_out[i % 2, 1] = total[half:]
        far(i, 0).start()
        far(i, 1).start()

    @pl.when((j >= 2) & (j <= tiles + 1))
    def _():
        i = j - 2
        far(i, 0).wait_recv()
        far(i, 1).wait_recv()

        @pl.when(i >= 2)
        def _():
            near(i - 2, 0).wait_send()
            near(i - 2, 1).wait_send()

        total = term(i, 4) + pair_in[i % 6, 2].astype(F32)
        near_out[i % 2, 0, :half] = total[:half].astype(BF16)
        near_out[i % 2, 0, half:] = (total[half:] + far_in[i % 4, 1].astype(F32)).astype(BF16)
        near(i, 0).start()
        total = term(i, 2) + pair_in[i % 6, 1].astype(F32)
        near_out[i % 2, 1, :half] = (total[:half] + far_in[i % 4, 0].astype(F32)).astype(BF16)
        near_out[i % 2, 1, half:] = total[half:].astype(BF16)
        near(i, 1).start()

    @pl.when(j >= 3)
    def _():
        i = j - 3
        total = dot(hs_ref[...], s_ref[...]) + term(i, 0) + pair_in[i % 6, 0].astype(F32)
        near(i, 0).wait_recv()
        near(i, 1).wait_recv()
        total = total + near_in[i % 4, 0].astype(F32) + near_in[i % 4, 1].astype(F32)
        y_ref[...] = total.astype(BF16)

    @pl.when(j < tiles)
    def _():
        for e in range(3, own):
            project(e)

        @pl.when(j >= 2)
        def _():
            pair(j - 2).wait_send()

        for q in range(n // 2):
            pair_out[j % 2, q] = term(j, 2 * q + 1).astype(BF16)
        pair(j).start()

    @pl.when(j == tiles + 2)
    def _():
        for i in (tiles - 2, tiles - 1):
            pair(i).wait_send()
            for k in range(2):
                far(i, k).wait_send()
                near(i, k).wait_send()


def down(here, away, slots, hs, w_down, s_down, pos, gate, tile):
    own, _, ff = here.shape
    n = pos.shape[1] // own
    rows = 2 * WIN + away.shape[1]
    tokens, depth = pos.shape[0], w_down.shape[2]
    tiles = depth // tile
    half = tokens // 2
    one = pl.Buffered(1)

    def whole(v):
        return pl.BlockSpec(v.shape, lambda j: (0,) * v.ndim, pipeline_mode=one)

    flops = 2 * own * rows * ff * depth
    dma = pltpu.SemaphoreType.DMA
    return pl.pallas_call(
        functools.partial(down_kernel, n, own, slots, tiles),
        out_shape=jax.ShapeDtypeStruct((tokens, depth), BF16),
        grid=(tiles + 3,),
        in_specs=[
            whole(pos),
            whole(gate),
            pl.BlockSpec(memory_space=pl.ANY),
            pl.BlockSpec(memory_space=pl.ANY),
            whole(hs),
            pl.BlockSpec((own, ff, tile), lambda j: (0, 0, jnp.minimum(j, tiles - 1))),
            pl.BlockSpec((s_down.shape[0], tile), lambda j: (0, jnp.maximum(j - 3, 0))),
        ],
        out_specs=pl.BlockSpec((tokens, tile), lambda j: (0, jnp.maximum(j - 3, 0))),
        scratch_shapes=[
            pltpu.VMEM((own, rows, ff), BF16),
            pltpu.VMEM((4, own, rows, tile), BF16),
            pltpu.VMEM((n, tokens, own * 128), BF16),
            pltpu.VMEM((2, n // 2, tokens, tile), BF16),
            pltpu.VMEM((6, n // 2, tokens, tile), BF16),
            pltpu.VMEM((2, 2, half, tile), BF16),
            pltpu.VMEM((4, 2, half, tile), BF16),
            pltpu.VMEM((2, 2, tokens, tile), BF16),
            pltpu.VMEM((4, 2, tokens, tile), BF16),
            dma((2,)),
            dma((6,)),
            dma((2, 2)),
            dma((4, 2)),
            dma((2, 2)),
            dma((4, 2)),
            dma((own, 2)),
        ],
        compiler_params=pltpu.CompilerParams(
            vmem_limit_bytes=VMEM_LIMIT, collective_id=0, has_side_effects=True
        ),
        cost_estimate=pl.CostEstimate(flops=flops, bytes_accessed=own * ff * depth * 2, transcendentals=0),
        name="down",
    )(pos, gate, here, away, hs, w_down, s_down)


def solution(mesh):
    n = mesh.shape["ep"]

    def local(x, expert, slot, gate, w_gate, w_up, w_down, s_gate, s_up, s_down):
        x, expert, slot, gate = x[0, 0], expert[0, 0], slot[0, 0], gate[0, 0]
        tokens, top = expert.shape
        own = w_gate.shape[0]
        experts = own * n
        slots = 5 * tokens * top // (4 * experts)

        hit = (expert[:, :, None] == jnp.arange(experts)) & (slot < slots)[:, :, None]
        pos = jnp.sum(jnp.where(hit, slot[:, :, None] + 1, 0), axis=1) - 1
        weight = jnp.sum(jnp.where(hit, gate.astype(BF16).astype(F32)[:, :, None], 0.0), axis=1)
        note = jnp.stack([pos.astype(F32), weight]).reshape(2, tokens, n, own).transpose(2, 0, 3, 1)
        note = jnp.pad(note.reshape(n, 2 * own, tokens), ((0, 0), (0, 8 - 2 * own), (0, 0)))
        hs, here, away, notes = up(x, note, slots, s_gate, s_up, w_gate, w_up)
        pos_col = notes[:, :own].reshape(n * own, tokens).T.astype(jnp.int32)
        weight = notes[:, own : 2 * own].reshape(n * own, tokens).T
        y = down(here, away, slots, hs, w_down, s_down, pos_col, weight, 512)
        return y[None, None]

    tok, exp, rep = P("dp", "ep"), P("ep"), P()
    return jax.shard_map(
        local,
        mesh=mesh,
        in_specs=(tok, tok, tok, tok, exp, exp, exp, rep, rep, rep),
        out_specs=tok,
        check_vma=False,
    )
```
